32 devices in a mesh: orb: 16 (over z, y, core), grid: 2 (over x).
Axes of the slice: x: 2, y: 2, z: 4, core: 2. Of those that a mesh axis runs over, the one named last changes fastest.
Arguments:
- orbitals: bfloat16 [32, 11520], P('orb', 'grid'), may hold values from -1.5 to 1.5
- occupation: bfloat16 [32], P('orb'), may hold values from 0.29882812 to 1
Outputs:
- potentials: float32 [32, 11520], P('orb', 'grid')
- projectors: float32 [32, 11520], P('orb', 'grid')
The draws below stay inside these ranges and needn't reach their ends.
All inputs are finite; a program needn't handle non-finite values.
Results may differ from the reference program's by a relative error of at most 0.0025.
Values may be sent and summed in bfloat16 or wider, within the bound.
No kernel may reach another device: no remote copies, remote signals or barrier semaphores. Data moves between devices by JAX's collectives and lax.ppermute only.
A program may use at most 64 MiB of HBM per device.

```python
import math
import jax
import jax.numpy as jnp
from jax import lax

NX = 20
NY = 24
NZ = 24
NORB = 32
NPTS = 11520


def shard_levels(rng, shape, split, smallest, top_value):
    def one(position, shards_of):
        heights = jax.random.uniform(jax.random.fold_in(jax.random.fold_in(rng, 6), position), (shards_of,), jnp.float32, smallest / len(split), top_value / len(split))
        return jnp.repeat(jnp.exp(heights), shape[position] // shards_of).reshape((-1,) + (1,) * (len(shape) - position - 1))

    factor_of = one(*split[0])
    for cut in split[1:]:
        factor_of = factor_of * one(*cut)
    return factor_of


def centred(own_key, extent, scale, bound, shards=(), held_as=jnp.bfloat16):
    array = jax.random.normal(own_key, extent, jnp.float32) * scale
    if len(shards) > 0:
        array = shard_levels(own_key, extent, shards, -0.22, 0.18) * array
    return jnp.clip(array, min=-bound, max=bound).astype(held_as)


def setup_inputs(seed: int = 0) -> dict:
    key_of = jax.random.split(jax.random.key(seed), 3)
    orbitals = centred(key_of[0], (NORB, NPTS), 0.25, 1.5, ((0, 16), (1, 2)))
    occupation = jnp.clip(0.29882812 + 0.7011719 * jax.random.uniform(key_of[1], (NORB,), jnp.float32) ** shard_levels(key_of[1], (NORB,), ((0, 16),), -0.2, 0.2), 0.29882812, 1.0).astype(jnp.bfloat16)
    return dict(orbitals=orbitals, occupation=occupation)


def hartley_table(length):
    index = jnp.arange(length, dtype=jnp.int32)
    product = index[:, None] * index[None, :] % length
    angle = 2.0 * math.pi / length * product.astype(jnp.float32)
    return (jnp.cos(angle) + jnp.sin(angle)).astype(jnp.bfloat16)

def signed_square(length):
    index = jnp.arange(length, dtype=jnp.int32)
    signed = jnp.where(index <= length // 2, index, index - length).astype(jnp.float32)
    return (2.0 * math.pi * signed / length) ** 2

def coulomb_kernel(size_x, size_y, size_z):
    total = signed_square(size_x)[:, None, None] + signed_square(size_y)[None, :, None] + signed_square(size_z)[None, None, :]
    safe = jnp.where(total > 0, total, 1.0)
    return jnp.where(total > 0, 1.0 / safe, 0.0) / (size_x * size_y * size_z)

def solve_pairs(density, table_x, table_y, table_z, kernel):
    fx = table_x.astype(jnp.float32)
    fy = table_y.astype(jnp.float32)
    fz = table_z.astype(jnp.float32)
    section = jnp.einsum('ax,pxyz->payz', fx, density.astype(jnp.float32)).astype(jnp.bfloat16)
    section = jnp.einsum('by,pxyz->pxbz', fy, section.astype(jnp.float32)).astype(jnp.bfloat16)
    spectrum = jnp.einsum('cz,pxyz->pxyc', fz, section.astype(jnp.float32))
    section = (spectrum * kernel).astype(jnp.bfloat16)
    section = jnp.einsum('cz,pxyz->pxyc', fz, section.astype(jnp.float32)).astype(jnp.bfloat16)
    section = jnp.einsum('by,pxyz->pxbz', fy, section.astype(jnp.float32)).astype(jnp.bfloat16)
    return jnp.einsum('ax,pxyz->payz', fx, section.astype(jnp.float32))

def reference(orbitals, occupation):
    table_x = hartley_table(NX)
    table_y = hartley_table(NY)
    table_z = hartley_table(NZ)
    kernel = coulomb_kernel(NX, NY, NZ)
    source = orbitals.astype(jnp.float32)
    weights = occupation.astype(jnp.float32)
    group = math.gcd(NORB, 32)
    blocks = source.reshape(NORB // group, group, NPTS)
    block_weights = weights.reshape(NORB // group, group)

    def potential_of(target):

        def accumulate(running, inputs):
            block, block_weight = inputs
            density = (target[None, :] * block).astype(jnp.bfloat16).reshape(group, NX, NY, NZ)
            potential = solve_pairs(density, table_x, table_y, table_z, kernel).reshape(group, NPTS)
            return (running - jnp.sum(block_weight[:, None] * potential * block, axis=0), None)
        running, unused = lax.scan(accumulate, jnp.zeros((NPTS,), jnp.float32), (blocks, block_weights))
        return running
    potentials = lax.map(potential_of, source)
    gram = lax.dot_general(source, potentials, (((1,), (1,)), ((), ())), precision=lax.Precision.HIGHEST) / NPTS
    factor = jnp.linalg.cholesky(-gram)
    inverse = lax.linalg.triangular_solve(factor, jnp.eye(NORB, dtype=jnp.float32), left_side=True, lower=True)
    projectors = jnp.dot(inverse, potentials, precision=lax.Precision.HIGHEST)
    return (potentials, projectors)
```

```python
import functools
import math

import jax
import jax.numpy as jnp
import numpy as np
from jax import lax
from jax.experimental import pallas as pl
from jax.experimental.pallas import tpu as pltpu
from jax.sharding import PartitionSpec as P

NX = 20
NY = 24
NZ = 24
NPTS = NX * NY * NZ
PLANE = NY * NZ
BAND = 128 // NZ
BANDS = -(-NY // BAND)
WIDE = BANDS * 128
F32 = jnp.float32
BF16 = jnp.bfloat16


def hartley_table(length):
    index = np.arange(length)
    angle = 2.0 * np.pi / length * (index[:, None] * index[None, :] % length)
    return (np.cos(angle) + np.sin(angle)).astype(BF16).astype(np.float32)


def signed_square(length):
    index = np.arange(length)
    signed = np.where(index <= length // 2, index, index - length)
    return (2.0 * np.pi * signed / length) ** 2


def coulomb_kernel():
    total = (
        signed_square(NX)[:, None, None]
        + signed_square(NY)[None, :, None]
        + signed_square(NZ)[None, None, :]
    )
    safe = np.where(total > 0, total, 1.0)
    return np.where(total > 0, 1.0 / safe, 0.0) / NPTS


def row_stride(own, planes):
    stride = planes + 1
    while own * stride % 8:
        stride += 1
    return stride


def tables(own, parts, cluster):
    planes = NX // parts
    stride = row_stride(own, planes)
    rows = own * stride
    table_x, table_y, table_z = hartley_table(NX), hartley_table(NY), hartley_table(NZ)
    mix_x = np.zeros((cluster, parts, own, stride, cluster, parts, own, stride), np.float32)
    cut = table_x.reshape(parts, planes, parts, planes)
    for owner in range(cluster):
        for orbital in range(own):
            mix_x[owner, :, orbital, :planes, owner, :, orbital, :planes] = cut
    mix_x = mix_x.reshape(cluster * parts * rows, cluster * parts * rows)
    lane = np.arange(NY)[:, None] // BAND * 128 + np.arange(NY)[:, None] % BAND * NZ + np.arange(NZ)
    mix_y = np.zeros((PLANE, WIDE), np.float32)
    natural = np.arange(PLANE).reshape(NY, NZ)
    for z in range(NZ):
        mix_y[np.ix_(natural[:, z], lane[:, z])] = table_y
    mix_z = np.zeros((256, 256), np.float32)
    for half in range(2):
        for band in range(BAND):
            at = half * 128 + band * NZ
            mix_z[at : at + NZ, at : at + NZ] = table_z
    scale = np.zeros((parts, own, stride, WIDE), np.float32)
    scale[:, :, :planes, lane.reshape(-1)] = coulomb_kernel().reshape(parts, 1, planes, PLANE)
    return (
        mix_x.astype(BF16),
        mix_y.astype(BF16),
        mix_z.astype(BF16),
        np.ascontiguousarray(mix_y.T).astype(BF16),
        scale.reshape(parts, rows, WIDE),
    )


def dot(left, right):
    return lax.dot_general(left, right, (((1,), (0,)), ((), ())), preferred_element_type=F32)


def bands(sections, mix_z):
    pieces = []
    for start in range(0, WIDE, 256):
        stop = min(start + 256, WIDE)
        width = stop - start
        pieces.append(dot(sections[:, start:stop], mix_z[:width, :width]))
    return jnp.concatenate(pieces, axis=1)


def halves(block, stride):
    return jnp.concatenate([block[..., stride:, :], block[..., :stride, :]], axis=-2)


def pair_body(
    place, blocks, mix_x, mix_y, mix_z, mix_back, scale, sent, totals,
    *, own, parts, stride, planes, cluster, chunk, copies,
):
    owners = blocks.shape[0] // parts
    rows = own * stride
    owner = place[0]
    part = place[1]
    row = lax.broadcasted_iota(jnp.int32, (1, rows, PLANE), 1)
    first = row < stride
    mine = blocks[pl.ds(owner * parts, parts)].astype(F32)
    target = jnp.where(first == (part == 0), mine, halves(mine, stride))
    totals[...] = jnp.zeros_like(totals)
    group = cluster * parts * rows
    x_table = mix_x[...]
    z_table = mix_z[...]

    def step(index, carry):
        source = blocks[pl.ds(index * chunk * parts, chunk * parts)].astype(F32)
        source = source.reshape(chunk, parts, rows, PLANE)
        density = (source * target[None]).astype(BF16).reshape(chunk * parts * rows, PLANE)
        section = jnp.concatenate(
            [
                dot(x_table, density[at : at + group]).astype(BF16)
                for at in range(0, chunk * parts * rows, group)
            ]
        )
        section = dot(section, mix_y[...]).astype(BF16)
        spectrum = bands(section, z_table).reshape(chunk, parts, rows, WIDE)
        section = (spectrum * scale[...][None]).astype(BF16).reshape(chunk * parts * rows, WIDE)
        section = bands(section, z_table).astype(BF16)
        section = dot(section, mix_back[...]).astype(BF16)
        potential = jnp.concatenate(
            [
                dot(x_table, section[at : at + group])
                for at in range(0, chunk * parts * rows, group)
            ]
        ).reshape(chunk, parts, rows, PLANE)
        weight = jnp.where(
            first[None],
            source[:, :, planes : planes + 1, :],
            source[:, :, stride + planes : stride + planes + 1, :],
        )
        totals[...] -= jnp.sum(weight * potential * source, axis=0)
        return carry

    steps = owners // chunk
    if steps == 1:
        step(0, 0)
    else:
        lax.fori_loop(0, steps, step, 0)
    partial = totals[...]
    folded = partial + halves(partial, stride)

    norb = owners * own
    lane = lax.broadcasted_iota(jnp.int32, (chunk, norb), 1)
    slot = lax.broadcasted_iota(jnp.int32, (chunk, norb), 0)

    def overlap(index, line):
        source = blocks[pl.ds(index * chunk * parts, chunk * parts)].astype(F32)
        source = source.reshape(chunk, parts, rows, PLANE)
        product = jnp.sum(source * folded[None], axis=1)
        for orbital in range(own):
            wanted = first if orbital == 0 else jnp.logical_not(first)
            picked = jnp.sum(jnp.where(wanted, product, 0.0), axis=1)
            value = jnp.sum(picked, axis=1, keepdims=True) / NPTS
            at = (index * chunk + slot) * own + orbital
            line = line + jnp.sum(jnp.where(lane == at, value, 0.0), axis=0, keepdims=True)
        return line

    line = jnp.zeros((1, norb), F32)
    line = overlap(0, line) if steps == 1 else lax.fori_loop(0, steps, overlap, line)
    line = jnp.concatenate([line, jnp.zeros((1, PLANE - norb), F32)], axis=1)
    sent_rows = sent.shape[2]
    place_row = lax.broadcasted_iota(jnp.int32, (1, sent_rows, PLANE), 1)
    mixed = jnp.where(place_row == planes, line[None], folded[:, :sent_rows])
    for at in range(copies):
        sent[at] = mixed


def solve_body(place, received, potentials, projectors, work, *, own, parts, planes):
    norb = received.shape[0]
    owner = place[0]
    gram = received[:, planes, :norb]
    matrix = -0.5 * (gram + gram.T)
    row = lax.broadcasted_iota(jnp.int32, (norb, norb), 0)
    column = lax.broadcasted_iota(jnp.int32, (norb, norb), 1)
    right = jnp.where(row == column, 1.0, 0.0).astype(F32)

    def eliminate(k, left, right, pivot_row, right_row, pivot_column):
        pivot = jnp.sum(jnp.where(column[:1] == k, pivot_row, 0.0), axis=1, keepdims=True)
        factor = jnp.where(row[:, :1] > k, pivot_column / pivot, 0.0)
        return left - factor * pivot_row, right - factor * right_row

    if norb <= 32:
        left = matrix
        for k in range(norb):
            factor = jnp.where(row[:, :1] > k, left[:, k : k + 1] / left[k : k + 1, k : k + 1], 0.0)
            left, right = left - factor * left[k : k + 1], right - factor * right[k : k + 1]
    else:
        work[0] = matrix
        work[1] = right

        def step(k, carry):
            left = work[0]
            right = work[1]
            pivot_row = work[0, pl.ds(k, 1), :]
            right_row = work[1, pl.ds(k, 1), :]
            pivot_column = jnp.sum(jnp.where(column == k, left, 0.0), axis=1, keepdims=True)
            work[0], work[1] = eliminate(k, left, right, pivot_row, right_row, pivot_column)
            return carry

        lax.fori_loop(0, norb, step, 0)
        left = work[0]
        right = work[1]
    diagonal = jnp.sum(jnp.where(row == column, left, 0.0), axis=1, keepdims=True)
    work[0] = right * lax.rsqrt(diagonal)
    for orbital in range(own):
        potentials[orbital] = received[owner * own + orbital, :planes, :]
        weights = work[0, pl.ds(owner * own + orbital, 1), :]
        total = jnp.zeros((planes, PLANE), F32)
        for at in range(norb):
            total = total + weights[:, at : at + 1] * received[at, :planes, :]
        projectors[orbital] = total


def on_device(orbitals, occupation):
    own = orbitals.shape[0]
    owners = lax.axis_size("orb")
    parts = lax.axis_size("grid")
    devices = owners * parts
    planes = NX // parts
    stride = row_stride(own, planes)
    rows = own * stride
    cluster = math.gcd(owners, max(1, 256 // (parts * rows)))
    chunk = math.gcd(owners, 16)
    place = jnp.stack([lax.axis_index("orb"), lax.axis_index("grid")]).astype(jnp.int32)
    block = jnp.concatenate(
        [
            orbitals.reshape(own, planes, PLANE),
            jnp.broadcast_to(occupation[:, None, None], (own, stride - planes, PLANE)),
        ],
        axis=1,
    ).reshape(1, rows, PLANE)
    blocks = spread(jnp.broadcast_to(block, (devices, rows, PLANE)))
    vmem = pl.BlockSpec(memory_space=pltpu.VMEM)
    smem = pl.BlockSpec(memory_space=pltpu.SMEM)
    sent_rows = 16
    sent = pl.pallas_call(
        functools.partial(
            pair_body, own=own, parts=parts, stride=stride, planes=planes,
            cluster=cluster, chunk=chunk, copies=owners,
        ),
        out_shape=jax.ShapeDtypeStruct((owners, parts, sent_rows, PLANE), F32),
        in_specs=[smem] + [vmem] * 6,
        out_specs=vmem,
        scratch_shapes=[pltpu.VMEM((parts, rows, PLANE), F32)],
        name="pairs",
    )(place, blocks, *(jnp.asarray(item) for item in tables(own, parts, cluster)))
    received = spread(sent.reshape(devices, sent_rows, PLANE))
    norb = owners * own
    shape = jax.ShapeDtypeStruct((own, planes, PLANE), F32)
    potentials, projectors = pl.pallas_call(
        functools.partial(solve_body, own=own, parts=parts, planes=planes),
        out_shape=(shape, shape),
        in_specs=[smem, vmem],
        out_specs=(vmem, vmem),
        scratch_shapes=[pltpu.VMEM((2, norb, norb), F32)],
        name="solve",
    )(place, received)
    size = planes * PLANE
    return (potentials.reshape(own, size), projectors.reshape(own, size))


def spread(blocks):
    return lax.all_to_all(blocks, ("orb", "grid"), split_axis=0, concat_axis=0, tiled=True)


def solution(mesh):
    placed = (P("orb", "grid"), P("orb"))
    return jax.shard_map(
        on_device,
        mesh=mesh,
        in_specs=placed,
        out_specs=(P("orb", "grid"), P("orb", "grid")),
        check_vma=False,
    )
```

```python
import functools
import math

import jax
import jax.numpy as jnp
import numpy as np
from jax import lax
from jax.experimental import pallas as pl
from jax.experimental.pallas import tpu as pltpu
from jax.sharding import PartitionSpec as P

NX = 20
NY = 24
NZ = 24
NPTS = NX * NY * NZ
PLANE = NY * NZ
BAND = 128 // NZ
BANDS = -(-NY // BAND)
WIDE = BANDS * 128
F32 = jnp.float32
BF16 = jnp.bfloat16


def hartley_table(length):
    index = np.arange(length)
    angle = 2.0 * np.pi / length * (index[:, None] * index[None, :] % length)
    return (np.cos(angle) + np.sin(angle)).astype(BF16).astype(np.float32)


def signed_square(length):
    index = np.arange(length)
    signed = np.where(index <= length // 2, index, index - length)
    return (2.0 * np.pi * signed / length) ** 2


def coulomb_kernel():
    total = (
        signed_square(NX)[:, None, None]
        + signed_square(NY)[None, :, None]
        + signed_square(NZ)[None, None, :]
    )
    safe = np.where(total > 0, total, 1.0)
    return np.where(total > 0, 1.0 / safe, 0.0) / NPTS


def row_stride(own, planes):
    stride = planes + 1
    while own * stride % 8:
        stride += 1
    return stride


def tables(own, parts, cluster):
    planes = NX // parts
    stride = row_stride(own, planes)
    rows = own * stride
    table_x, table_y, table_z = hartley_table(NX), hartley_table(NY), hartley_table(NZ)
    mix_x = np.zeros((parts,) + (parts, cluster, own, stride) * 2, np.float32)
    cut = table_x.reshape(parts, planes, parts, planes)
    for part in range(parts):
        order = [part ^ other for other in range(parts)]
        for owner in range(cluster):
            for orbital in range(own):
                mix_x[part, :, owner, orbital, :planes, :, owner, orbital, :planes] = cut[
                    order
                ][:, :, order].transpose(0, 1, 2, 3)
    mix_x = mix_x.reshape(parts, cluster * parts * rows, cluster * parts * rows)
    lane = np.arange(NY)[:, None] // BAND * 128 + np.arange(NY)[:, None] % BAND * NZ + np.arange(NZ)
    mix_y = np.zeros((PLANE, WIDE), np.float32)
    natural = np.arange(PLANE).reshape(NY, NZ)
    for z in range(NZ):
        mix_y[np.ix_(natural[:, z], lane[:, z])] = table_y
    mix_z = np.zeros((256, 256), np.float32)
    for half in range(2):
        for band in range(BAND):
            at = half * 128 + band * NZ
            mix_z[at : at + NZ, at : at + NZ] = table_z
    scale = np.zeros((parts, own, stride, WIDE), np.float32)
    scale[:, :, :planes, lane.reshape(-1)] = coulomb_kernel().reshape(parts, 1, planes, PLANE)
    return (
        mix_x.astype(BF16),
        mix_y.astype(BF16),
        mix_z.astype(BF16),
        np.ascontiguousarray(mix_y.T).astype(BF16),
        scale.reshape(parts, rows, WIDE),
    )


def dot(left, right):
    return lax.dot_general(left, right, (((1,), (0,)), ((), ())), preferred_element_type=F32)


def bands(sections, mix_z):
    pieces = []
    for start in range(0, WIDE, 256):
        stop = min(start + 256, WIDE)
        width = stop - start
        pieces.append(dot(sections[:, start:stop], mix_z[:width, :width]))
    return jnp.concatenate(pieces, axis=1)


def halves(block, stride):
    return jnp.concatenate([block[..., stride:, :], block[..., :stride, :]], axis=-2)


class Route:
    def __init__(self, devices):
        top = devices.bit_length() - 1
        rest = list(range(top - 1, 1, -1))
        rounds = [rest[:2], rest[2:3] + [0]]
        rounds += [rest[at : at + 2] for at in range(3, len(rest), 2)] + [[1]]
        self.devices = devices
        self.rounds = rounds
        self.bits = [bit for members in rounds for bit in reversed(members)]
        self.owner_bits = [bit - 1 for bit in self.bits if bit]
        self.cluster = 1 << len(rounds[0])

    def masks(self, members):
        order = list(reversed(members))
        return [
            sum((at >> t & 1) << bit for t, bit in enumerate(order))
            for at in range(1 << len(order))
        ]

    def swap(self, array, mask):
        pairs = [(at, at ^ mask) for at in range(self.devices)]
        return lax.ppermute(array, ("orb", "grid"), pairs)


def spell(position, bits):
    return sum((position >> t & 1) << bit for t, bit in enumerate(bits))


def pack_body(orbitals, occupation, block, *, own, planes, stride):
    values = orbitals[...].astype(F32)
    weights = occupation[...].astype(F32)
    lines = []
    for orbital in range(own):
        for x in range(planes):
            lines.append(values[orbital : orbital + 1, x * PLANE : (x + 1) * PLANE])
        lines.append(
            jnp.broadcast_to(weights[orbital : orbital + 1], (stride - planes, PLANE))
        )
    block[0] = jnp.concatenate(lines, axis=0).astype(BF16)


def target_of(part, local, own, stride, cluster):
    mine = jnp.stack([local[0], local[cluster]]).astype(F32)
    first = lax.broadcasted_iota(jnp.int32, mine.shape, 1) < stride
    return jnp.where(first == (part == 0), mine, halves(mine, stride))


def sources_of(blocks, index, chunk, parts, cluster):
    source = blocks[pl.ds(index * chunk, chunk)].astype(F32)
    return source.reshape((chunk // (parts * cluster), parts, cluster) + blocks.shape[1:])


def add_pairs(
    part, target, blocks, mix_x, mix_y, mix_z, mix_back, scale, totals,
    *, parts, stride, planes, cluster, chunk,
):
    rows = blocks.shape[1]
    group = parts * cluster * rows
    first = lax.broadcasted_iota(jnp.int32, (1, 1, 1, rows, PLANE), 3) < stride
    x_table = mix_x[part]
    z_table = mix_z[...]
    factor = jnp.stack([scale[part], scale[1 - part]])[None, :, None]

    def step(index, carry):
        source = sources_of(blocks, index, chunk, parts, cluster)
        shape = source.shape[:-1]
        height = chunk * rows
        density = (source * target[None, :, None]).astype(BF16).reshape(height, PLANE)
        section = jnp.concatenate(
            [
                dot(x_table, density[at : at + group]).astype(BF16)
                for at in range(0, height, group)
            ]
        )
        section = dot(section, mix_y[...]).astype(BF16)
        spectrum = bands(section, z_table).reshape(shape + (WIDE,))
        section = (spectrum * factor).astype(BF16).reshape(height, WIDE)
        section = bands(section, z_table).astype(BF16)
        section = dot(section, mix_back[...]).astype(BF16)
        potential = jnp.concatenate(
            [dot(x_table, section[at : at + group]) for at in range(0, height, group)]
        ).reshape(shape + (PLANE,))
        weight = jnp.where(
            first,
            source[..., planes : planes + 1, :],
            source[..., stride + planes : stride + planes + 1, :],
        )
        totals[...] -= jnp.sum(weight * potential * source, axis=(0, 2))
        return carry

    steps = blocks.shape[0] // chunk
    if steps == 1:
        step(0, 0)
    else:
        lax.fori_loop(0, steps, step, 0)


def first_body(place, local, mix_x, mix_y, mix_z, mix_back, scale, totals, *, own, **sizes):
    target = target_of(place[1], local, own, sizes["stride"], sizes["cluster"])
    totals[...] = jnp.zeros_like(totals)
    add_pairs(
        place[1], target, local, mix_x, mix_y, mix_z, mix_back, scale, totals, **sizes
    )


def second_body(
    place, local, other, mix_x, mix_y, mix_z, mix_back, scale, before, sent, kept, totals,
    *, own, owner_bits, **sizes,
):
    stride, planes = sizes["stride"], sizes["planes"]
    parts, cluster, chunk = sizes["parts"], sizes["cluster"], sizes["chunk"]
    target = target_of(place[1], local, own, stride, cluster)
    totals[...] = before[...]
    add_pairs(
        place[1], target, other, mix_x, mix_y, mix_z, mix_back, scale, totals, **sizes
    )
    partial = totals[...]
    folded = partial + halves(partial, stride)
    rows = own * stride
    count = chunk // parts
    half = local.shape[0] // parts
    norb = 2 * half * own
    lane = lax.broadcasted_iota(jnp.int32, (count, norb), 1)
    slot = lax.broadcasted_iota(jnp.int32, (count, norb), 0)
    first = lax.broadcasted_iota(jnp.int32, (count, rows, PLANE), 1) < stride

    def overlap(blocks, base):
        def step(index, line):
            source = sources_of(blocks, index, chunk, parts, cluster)
            product = jnp.sum(source * folded[None, :, None], axis=1).reshape(count, rows, PLANE)
            owner = spell(base + index * count + slot, owner_bits) ^ place[0]
            for orbital in range(own):
                wanted = first if orbital == 0 else jnp.logical_not(first)
                picked = jnp.sum(jnp.where(wanted, product, 0.0), axis=1)
                value = jnp.sum(picked, axis=1, keepdims=True) / NPTS
                at = owner * own + orbital
                line = line + jnp.sum(jnp.where(lane == at, value, 0.0), axis=0, keepdims=True)
            return line

        return step

    line = jnp.zeros((1, norb), F32)
    steps = local.shape[0] // chunk
    for blocks, base in ((local, 0), (other, half)):
        step = overlap(blocks, base)
        line = step(0, line) if steps == 1 else lax.fori_loop(0, steps, step, line)
    line = jnp.concatenate([line, jnp.zeros((1, PLANE - norb), F32)], axis=1)
    high = line.astype(BF16).astype(F32)
    middle = (line - high).astype(BF16).astype(F32)
    low = line - high - middle
    height = sent.shape[1]
    row = lax.broadcasted_iota(jnp.int32, (1, height, PLANE), 1)
    mixed = folded[:, :height]
    for at, value in enumerate((high, middle, low)):
        mixed = jnp.where(row == planes + at, value[None], mixed)
    sent[...] = mixed.astype(BF16)
    kept[...] = folded[:, :height]


def solve_body(
    place, local, other, kept, partner, potentials, projectors, lines, work, weights,
    *, own, planes, bits, cluster,
):
    norb = lines.shape[0]
    half = norb // 2
    me = place[2]
    for blocks, base in ((local, 0), (other, half)):
        raw = blocks[:, :, :norb].astype(F32)
        lines[base : base + half] = (
            raw[:, planes] + raw[:, planes + 1] + raw[:, planes + 2]
        )

    def repeat(step):
        if norb <= 32:
            for at in range(norb):
                step(at)
        else:
            lax.fori_loop(0, norb, lambda at, carry: (step(at), carry)[1], 0)

    def settle(at):
        work[0, pl.ds(spell(at, bits) ^ me, 1), :] = lines[pl.ds(at, 1), :]

    repeat(settle)
    gram = work[0]
    left = -0.5 * (gram + gram.T)
    row = lax.broadcasted_iota(jnp.int32, (norb, norb), 0)
    column = lax.broadcasted_iota(jnp.int32, (norb, norb), 1)
    right = jnp.where(row == column, 1.0, 0.0).astype(F32)
    if norb <= 32:
        for k in range(norb):
            factor = jnp.where(row[:, :1] > k, left[:, k : k + 1] / left[k : k + 1, k : k + 1], 0.0)
            left, right = left - factor * left[k : k + 1], right - factor * right[k : k + 1]
    else:
        work[0] = left
        work[1] = right

        def step(k, carry):
            left = work[0]
            pivot_row = work[0, pl.ds(k, 1), :]
            right_row = work[1, pl.ds(k, 1), :]
            pivot = jnp.sum(jnp.where(column[:1] == k, pivot_row, 0.0), axis=1, keepdims=True)
            below = jnp.sum(jnp.where(column == k, left, 0.0), axis=1, keepdims=True)
            factor = jnp.where(row[:, :1] > k, below / pivot, 0.0)
            work[0] = left - factor * pivot_row
            work[1] = work[1] - factor * right_row
            return carry

        lax.fori_loop(0, norb, step, 0)
        left = work[0]
        right = work[1]
    diagonal = jnp.sum(jnp.where(row == column, left, 0.0), axis=1, keepdims=True)
    turned = (right * lax.rsqrt(diagonal)).T
    for orbital in range(own):
        at = place[0] * own + orbital
        value = jnp.sum(jnp.where(column == at, turned, 0.0), axis=1, keepdims=True)
        weights[orbital] = jnp.broadcast_to(value, (norb, PLANE))

    height = local.shape[1]
    own_values = kept[0]
    partner_values = partner[...]
    start = []
    for orbital in range(own):
        start.append(
            weights[orbital, pl.ds(me, 1), :] * (own_values - local[0].astype(F32))
            + weights[orbital, pl.ds(me ^ 1, 1), :]
            * (partner_values - local[cluster].astype(F32))
        )

    def gather(blocks, base):
        def step(at, sums):
            value = blocks[at].astype(F32)
            where = spell(base + at, bits) ^ me
            return tuple(
                sums[orbital] + weights[orbital, pl.ds(where, 1), :] * value
                for orbital in range(own)
            )

        return step

    sums = tuple(start)
    for blocks, base in ((local, 0), (other, half)):
        step = gather(blocks, base)
        if norb <= 32:
            for at in range(half):
                sums = step(at, sums)
        else:
            sums = lax.fori_loop(0, half, step, sums)
    second = place[1] == 1
    for orbital in range(own):
        swapped = second if orbital == 0 else jnp.logical_not(second)
        value = jnp.where(swapped, partner_values, own_values)
        for x in range(planes):
            lanes = slice(x * PLANE, (x + 1) * PLANE)
            potentials[orbital : orbital + 1, lanes] = value[x : x + 1]
            projectors[orbital : orbital + 1, lanes] = sums[orbital][x : x + 1]


def on_device(orbitals, occupation):
    own = orbitals.shape[0]
    owners = lax.axis_size("orb")
    parts = lax.axis_size("grid")
    devices = owners * parts
    planes = NX // parts
    stride = row_stride(own, planes)
    rows = own * stride
    route = Route(devices)
    cluster = route.cluster
    sizes = dict(parts=parts, stride=stride, planes=planes, cluster=cluster, chunk=16)
    orb, grid = lax.axis_index("orb"), lax.axis_index("grid")
    place = jnp.stack([orb, grid, orb * parts + grid]).astype(jnp.int32)
    vmem = pl.BlockSpec(memory_space=pltpu.VMEM)
    smem = pl.BlockSpec(memory_space=pltpu.SMEM)
    shape = jax.ShapeDtypeStruct
    mixing = [jnp.asarray(item) for item in tables(own, parts, cluster)]

    local = pl.pallas_call(
        functools.partial(pack_body, own=own, planes=planes, stride=stride),
        out_shape=shape((1, rows, PLANE), BF16),
        in_specs=[vmem, vmem],
        out_specs=vmem,
        name="pack",
    )(orbitals, occupation.reshape(own, 1))
    for members in route.rounds[:-1]:
        local = jnp.concatenate(
            [local] + [route.swap(local, mask) for mask in route.masks(members)[1:]]
        )
    other = route.swap(local, route.masks(route.rounds[-1])[1])

    totals_shape = (parts, rows, PLANE)
    before = pl.pallas_call(
        functools.partial(first_body, own=own, **sizes),
        out_shape=shape(totals_shape, F32),
        in_specs=[smem] + [vmem] * 6,
        out_specs=vmem,
        name="near_pairs",
    )(place, local, *mixing)
    height = 16
    sent, kept = pl.pallas_call(
        functools.partial(second_body, own=own, owner_bits=route.owner_bits, **sizes),
        out_shape=(shape((parts, height, PLANE), BF16), shape((parts, height, PLANE), F32)),
        in_specs=[smem] + [vmem] * 8,
        out_specs=(vmem, vmem),
        scratch_shapes=[pltpu.VMEM(totals_shape, F32)],
        name="far_pairs",
    )(place, local, other, *mixing, before)

    column = sent[:, None]
    column = jnp.concatenate(
        [column] + [route.swap(column, mask) for mask in route.masks(route.rounds[0])[1:]], axis=1
    )
    partner = route.swap(kept[1], 1)
    near, far = column[0], column[1]
    near = jnp.concatenate(
        [near]
        + [route.swap(far if mask & 1 else near, mask) for mask in route.masks(route.rounds[1])[1:]]
    )
    for members in route.rounds[2:-1]:
        near = jnp.concatenate(
            [near] + [route.swap(near, mask) for mask in route.masks(members)[1:]]
        )
    away = route.swap(near, route.masks(route.rounds[-1])[1])
    norb = devices
    size = planes * PLANE
    return tuple(
        pl.pallas_call(
            functools.partial(
                solve_body, own=own, planes=planes, bits=route.bits, cluster=cluster
            ),
            out_shape=(shape((own, size), F32), shape((own, size), F32)),
            in_specs=[smem] + [vmem] * 4,
            out_specs=(vmem, vmem),
            scratch_shapes=[
                pltpu.VMEM((norb, norb), F32),
                pltpu.VMEM((2, norb, norb), F32),
                pltpu.VMEM((own, norb, PLANE), F32),
            ],
            name="solve",
        )(place, near, away, kept, partner)
    )


def solution(mesh):
    placed = (P("orb", "grid"), P("orb"))
    return jax.shard_map(
        on_device,
        mesh=mesh,
        in_specs=placed,
        out_specs=(P("orb", "grid"), P("orb", "grid")),
        check_vma=False,
    )
```

```python
import functools
import math

import jax
import jax.numpy as jnp
import numpy as np
from jax import lax
from jax.experimental import pallas as pl
from jax.experimental.pallas import tpu as pltpu
from jax.sharding import PartitionSpec as P

NX = 20
NY = 24
NZ = 24
NPTS = NX * NY * NZ
PLANE = NY * NZ
BAND = 128 // NZ
BANDS = -(-NY // BAND)
WIDE = BANDS * 128
F32 = jnp.float32
BF16 = jnp.bfloat16


def hartley_table(length):
    index = np.arange(length)
    angle = 2.0 * np.pi / length * (index[:, None] * index[None, :] % length)
    return (np.cos(angle) + np.sin(angle)).astype(BF16).astype(np.float32)


def signed_square(length):
    index = np.arange(length)
    signed = np.where(index <= length // 2, index, index - length)
    return (2.0 * np.pi * signed / length) ** 2


def coulomb_kernel():
    total = (
        signed_square(NX)[:, None, None]
        + signed_square(NY)[None, :, None]
        + signed_square(NZ)[None, None, :]
    )
    safe = np.where(total > 0, total, 1.0)
    return np.where(total > 0, 1.0 / safe, 0.0) / NPTS


def row_stride(own, planes):
    stride = planes + 1
    while own * stride % 8:
        stride += 1
    return stride


def tables(own, parts, cluster):
    planes = NX // parts
    stride = row_stride(own, planes)
    rows = own * stride
    table_x, table_y, table_z = hartley_table(NX), hartley_table(NY), hartley_table(NZ)
    mix_x = np.zeros((parts,) + (parts, cluster, own, stride) * 2, np.float32)
    cut = table_x.reshape(parts, planes, parts, planes)
    for part in range(parts):
        order = [part ^ other for other in range(parts)]
        for owner in range(cluster):
            for orbital in range(own):
                mix_x[part, :, owner, orbital, :planes, :, owner, orbital, :planes] = cut[
                    order
                ][:, :, order].transpose(0, 1, 2, 3)
    mix_x = mix_x.reshape(parts, cluster * parts * rows, cluster * parts * rows)
    lane = np.arange(NY)[:, None] // BAND * 128 + np.arange(NY)[:, None] % BAND * NZ + np.arange(NZ)
    mix_y = np.zeros((PLANE, WIDE), np.float32)
    natural = np.arange(PLANE).reshape(NY, NZ)
    for z in range(NZ):
        mix_y[np.ix_(natural[:, z], lane[:, z])] = table_y
    mix_z = np.zeros((256, 256), np.float32)
    for half in range(2):
        for band in range(BAND):
            at = half * 128 + band * NZ
            mix_z[at : at + NZ, at : at + NZ] = table_z
    scale = np.zeros((parts, own, stride, WIDE), np.float32)
    scale[:, :, :planes, lane.reshape(-1)] = coulomb_kernel().reshape(parts, 1, planes, PLANE)
    return (
        mix_x.astype(BF16),
        mix_y.astype(BF16),
        mix_z.astype(BF16),
        np.ascontiguousarray(mix_y.T).astype(BF16),
        scale.reshape(parts, rows, WIDE),
    )


def dot(left, right):
    return lax.dot_general(left, right, (((1,), (0,)), ((), ())), preferred_element_type=F32)


def bands(sections, mix_z):
    pieces = []
    for start in range(0, WIDE, 256):
        stop = min(start + 256, WIDE)
        width = stop - start
        pieces.append(dot(sections[:, start:stop], mix_z[:width, :width]))
    return jnp.concatenate(pieces, axis=1)


def halves(block, stride):
    return jnp.concatenate([block[..., stride:, :], block[..., :stride, :]], axis=-2)


class Route:
    def __init__(self, devices):
        top = devices.bit_length() - 1
        rest = list(range(top - 1, 1, -1))
        rounds = [rest[:2][::-1], rest[2:3] + [0]]
        rounds += [rest[at : at + 2] for at in range(3, len(rest), 2)] + [[1]]
        self.devices = devices
        self.rounds = rounds
        self.bits = [bit for members in rounds for bit in reversed(members)]
        self.owner_bits = [bit - 1 for bit in self.bits if bit]
        self.cluster = 1 << len(rounds[0])

    def masks(self, members):
        order = list(reversed(members))
        return [
            sum((at >> t & 1) << bit for t, bit in enumerate(order))
            for at in range(1 << len(order))
        ]

    def swap(self, array, mask):
        pairs = [(at, at ^ mask) for at in range(self.devices)]
        return lax.ppermute(array, ("orb", "grid"), pairs)


def spell(position, bits):
    return sum((position >> t & 1) << bit for t, bit in enumerate(bits))


def pack_body(orbitals, occupation, block, *, own, planes, stride):
    values = orbitals[...].astype(F32)
    weights = occupation[...].astype(F32)
    lines = []
    for orbital in range(own):
        for x in range(planes):
            lines.append(values[orbital : orbital + 1, x * PLANE : (x + 1) * PLANE])
        lines.append(
            jnp.broadcast_to(weights[orbital : orbital + 1], (stride - planes, PLANE))
        )
    block[0] = jnp.concatenate(lines, axis=0).astype(BF16)


def target_of(part, local, own, stride, cluster):
    mine = jnp.stack([local[0], local[cluster]]).astype(F32)
    first = lax.broadcasted_iota(jnp.int32, mine.shape, 1) < stride
    return jnp.where(first == (part == 0), mine, halves(mine, stride))


def sources_of(blocks, index, chunk, parts, cluster):
    source = blocks[pl.ds(index * chunk, chunk)].astype(F32)
    return source.reshape((chunk // (parts * cluster), parts, cluster) + blocks.shape[1:])


def add_pairs(
    part, target, blocks, mix_x, mix_y, mix_z, mix_back, scale, totals,
    *, parts, stride, planes, cluster, chunk,
):
    rows = blocks.shape[1]
    group = parts * cluster * rows
    first = lax.broadcasted_iota(jnp.int32, (1, 1, 1, rows, PLANE), 3) < stride
    x_table = mix_x[part]
    z_table = mix_z[...]
    factor = jnp.stack([scale[part], scale[1 - part]])[None, :, None]

    def step(index, carry):
        source = sources_of(blocks, index, chunk, parts, cluster)
        shape = source.shape[:-1]
        height = chunk * rows
        density = (source * target[None, :, None]).astype(BF16).reshape(height, PLANE)
        section = jnp.concatenate(
            [
                dot(x_table, density[at : at + group]).astype(BF16)
                for at in range(0, height, group)
            ]
        )
        section = dot(section, mix_y[...]).astype(BF16)
        spectrum = bands(section, z_table).reshape(shape + (WIDE,))
        section = (spectrum * factor).astype(BF16).reshape(height, WIDE)
        section = bands(section, z_table).astype(BF16)
        section = dot(section, mix_back[...]).astype(BF16)
        potential = jnp.concatenate(
            [dot(x_table, section[at : at + group]) for at in range(0, height, group)]
        ).reshape(shape + (PLANE,))
        weight = jnp.where(
            first,
            source[..., planes : planes + 1, :],
            source[..., stride + planes : stride + planes + 1, :],
        )
        totals[...] -= jnp.sum(weight * potential * source, axis=(0, 2))
        return carry

    steps = blocks.shape[0] // chunk
    if steps == 1:
        step(0, 0)
    else:
        lax.fori_loop(0, steps, step, 0)


def first_body(place, local, mix_x, mix_y, mix_z, mix_back, scale, totals, *, own, **sizes):
    target = target_of(place[1], local, own, sizes["stride"], sizes["cluster"])
    totals[...] = jnp.zeros_like(totals)
    add_pairs(
        place[1], target, local, mix_x, mix_y, mix_z, mix_back, scale, totals, **sizes
    )


def second_body(
    place, local, other, mix_x, mix_y, mix_z, mix_back, scale, before, sent, kept, totals,
    *, own, owner_bits, **sizes,
):
    stride, planes = sizes["stride"], sizes["planes"]
    parts, cluster, chunk = sizes["parts"], sizes["cluster"], sizes["chunk"]
    target = target_of(place[1], local, own, stride, cluster)
    totals[...] = before[...]
    add_pairs(
        place[1], target, other, mix_x, mix_y, mix_z, mix_back, scale, totals, **sizes
    )
    partial = totals[...]
    folded = partial + halves(partial, stride)
    rows = own * stride
    count = chunk // parts
    half = local.shape[0] // parts
    norb = 2 * half * own
    lane = lax.broadcasted_iota(jnp.int32, (count, norb), 1)
    slot = lax.broadcasted_iota(jnp.int32, (count, norb), 0)
    first = lax.broadcasted_iota(jnp.int32, (count, rows, PLANE), 1) < stride

    def overlap(blocks, base):
        def step(index, line):
            source = sources_of(blocks, index, chunk, parts, cluster)
            product = jnp.sum(source * folded[None, :, None], axis=1).reshape(count, rows, PLANE)
            owner = spell(base + index * count + slot, owner_bits) ^ place[0]
            for orbital in range(own):
                wanted = first if orbital == 0 else jnp.logical_not(first)
                picked = jnp.sum(jnp.where(wanted, product, 0.0), axis=1)
                value = jnp.sum(picked, axis=1, keepdims=True) / NPTS
                at = owner * own + orbital
                line = line + jnp.sum(jnp.where(lane == at, value, 0.0), axis=0, keepdims=True)
            return line

        return step

    line = jnp.zeros((1, norb), F32)
    steps = local.shape[0] // chunk
    for blocks, base in ((local, 0), (other, half)):
        step = overlap(blocks, base)
        line = step(0, line) if steps == 1 else lax.fori_loop(0, steps, step, line)
    line = jnp.concatenate([line, jnp.zeros((1, PLANE - norb), F32)], axis=1)
    high = line.astype(BF16).astype(F32)
    middle = (line - high).astype(BF16).astype(F32)
    low = line - high - middle
    height = sent.shape[1]
    row = lax.broadcasted_iota(jnp.int32, (1, height, PLANE), 1)
    mixed = folded[:, :height]
    for at, value in enumerate((high, middle, low)):
        mixed = jnp.where(row == planes + at, value[None], mixed)
    sent[...] = mixed.astype(BF16)
    kept[...] = folded[:, :height]


def solve_body(
    place, local, other, kept, partner, potentials, projectors, lines, work, weights,
    *, own, planes, bits, cluster,
):
    norb = lines.shape[0]
    half = norb // 2
    me = place[2]
    for blocks, base in ((local, 0), (other, half)):
        raw = blocks[:, :, :norb].astype(F32)
        lines[base : base + half] = (
            raw[:, planes] + raw[:, planes + 1] + raw[:, planes + 2]
        )

    def repeat(step):
        if norb <= 32:
            for at in range(norb):
                step(at)
        else:
            lax.fori_loop(0, norb, lambda at, carry: (step(at), carry)[1], 0)

    def settle(at):
        work[0, pl.ds(spell(at, bits) ^ me, 1), :] = lines[pl.ds(at, 1), :]

    repeat(settle)
    gram = work[0]
    left = -0.5 * (gram + gram.T)
    row = lax.broadcasted_iota(jnp.int32, (norb, norb), 0)
    column = lax.broadcasted_iota(jnp.int32, (norb, norb), 1)
    right = jnp.where(row == column, 1.0, 0.0).astype(F32)
    if norb <= 32:
        for k in range(norb):
            factor = jnp.where(row[:, :1] > k, left[:, k : k + 1] / left[k : k + 1, k : k + 1], 0.0)
            left, right = left - factor * left[k : k + 1], right - factor * right[k : k + 1]
    else:
        work[0] = left
        work[1] = right

        def step(k, carry):
            left = work[0]
            pivot_row = work[0, pl.ds(k, 1), :]
            right_row = work[1, pl.ds(k, 1), :]
            pivot = jnp.sum(jnp.where(column[:1] == k, pivot_row, 0.0), axis=1, keepdims=True)
            below = jnp.sum(jnp.where(column == k, left, 0.0), axis=1, keepdims=True)
            factor = jnp.where(row[:, :1] > k, below / pivot, 0.0)
            work[0] = left - factor * pivot_row
            work[1] = work[1] - factor * right_row
            return carry

        lax.fori_loop(0, norb, step, 0)
        left = work[0]
        right = work[1]
    diagonal = jnp.sum(jnp.where(row == column, left, 0.0), axis=1, keepdims=True)
    turned = (right * lax.rsqrt(diagonal)).T
    for orbital in range(own):
        at = place[0] * own + orbital
        value = jnp.sum(jnp.where(column == at, turned, 0.0), axis=1, keepdims=True)
        weights[orbital] = jnp.broadcast_to(value, (norb, PLANE))

    height = local.shape[1]
    own_values = kept[0]
    partner_values = partner[...]
    start = []
    for orbital in range(own):
        start.append(
            weights[orbital, pl.ds(me, 1), :] * (own_values - local[0].astype(F32))
            + weights[orbital, pl.ds(me ^ 1, 1), :]
            * (partner_values - local[cluster].astype(F32))
        )

    def gather(blocks, base):
        def step(at, sums):
            value = blocks[at].astype(F32)
            where = spell(base + at, bits) ^ me
            return tuple(
                sums[orbital] + weights[orbital, pl.ds(where, 1), :] * value
                for orbital in range(own)
            )

        return step

    sums = tuple(start)
    for blocks, base in ((local, 0), (other, half)):
        step = gather(blocks, base)
        if norb <= 32:
            for at in range(half):
                sums = step(at, sums)
        else:
            sums = lax.fori_loop(0, half, step, sums)
    second = place[1] == 1
    for orbital in range(own):
        swapped = second if orbital == 0 else jnp.logical_not(second)
        value = jnp.where(swapped, partner_values, own_values)
        for x in range(planes):
            lanes = slice(x * PLANE, (x + 1) * PLANE)
            potentials[orbital : orbital + 1, lanes] = value[x : x + 1]
            projectors[orbital : orbital + 1, lanes] = sums[orbital][x : x + 1]


def on_device(orbitals, occupation):
    own = orbitals.shape[0]
    owners = lax.axis_size("orb")
    parts = lax.axis_size("grid")
    devices = owners * parts
    planes = NX // parts
    stride = row_stride(own, planes)
    rows = own * stride
    route = Route(devices)
    cluster = route.cluster
    sizes = dict(parts=parts, stride=stride, planes=planes, cluster=cluster, chunk=16)
    orb, grid = lax.axis_index("orb"), lax.axis_index("grid")
    place = jnp.stack([orb, grid, orb * parts + grid]).astype(jnp.int32)
    vmem = pl.BlockSpec(memory_space=pltpu.VMEM)
    smem = pl.BlockSpec(memory_space=pltpu.SMEM)
    shape = jax.ShapeDtypeStruct
    mixing = [jnp.asarray(item) for item in tables(own, parts, cluster)]

    local = pl.pallas_call(
        functools.partial(pack_body, own=own, planes=planes, stride=stride),
        out_shape=shape((1, rows, PLANE), BF16),
        in_specs=[vmem, vmem],
        out_specs=vmem,
        name="pack",
    )(orbitals, occupation.reshape(own, 1))
    for bit in reversed(route.rounds[0]):
        local = jnp.concatenate([local, route.swap(local, 1 << bit)])
    for members in route.rounds[1:-1]:
        local = jnp.concatenate(
            [local] + [route.swap(local, mask) for mask in route.masks(members)[1:]]
        )
    other = route.swap(local, route.masks(route.rounds[-1])[1])

    totals_shape = (parts, rows, PLANE)
    before = pl.pallas_call(
        functools.partial(first_body, own=own, **sizes),
        out_shape=shape(totals_shape, F32),
        in_specs=[smem] + [vmem] * 6,
        out_specs=vmem,
        name="near_pairs",
    )(place, local, *mixing)
    height = 16
    sent, kept = pl.pallas_call(
        functools.partial(second_body, own=own, owner_bits=route.owner_bits, **sizes),
        out_shape=(shape((parts, height, PLANE), BF16), shape((parts, height, PLANE), F32)),
        in_specs=[smem] + [vmem] * 8,
        out_specs=(vmem, vmem),
        scratch_shapes=[pltpu.VMEM(totals_shape, F32)],
        name="far_pairs",
    )(place, local, other, *mixing, before)

    column = sent[:, None]
    column = jnp.concatenate(
        [column] + [route.swap(column, mask) for mask in route.masks(route.rounds[0])[1:]], axis=1
    )
    partner = route.swap(kept[1], 1)
    column, partner = lax.optimization_barrier((column, partner))
    near, far = column[0], column[1]
    near = jnp.concatenate(
        [near]
        + [route.swap(far if mask & 1 else near, mask) for mask in route.masks(route.rounds[1])[1:]]
    )
    for members in route.rounds[2:-1]:
        near = jnp.concatenate(
            [near] + [route.swap(near, mask) for mask in route.masks(members)[1:]]
        )
    away = route.swap(near, route.masks(route.rounds[-1])[1])
    norb = devices
    size = planes * PLANE
    return tuple(
        pl.pallas_call(
            functools.partial(
                solve_body, own=own, planes=planes, bits=route.bits, cluster=cluster
            ),
            out_shape=(shape((own, size), F32), shape((own, size), F32)),
            in_specs=[smem] + [vmem] * 4,
            out_specs=(vmem, vmem),
            scratch_shapes=[
                pltpu.VMEM((norb, norb), F32),
                pltpu.VMEM((2, norb, norb), F32),
                pltpu.VMEM((own, norb, PLANE), F32),
            ],
            name="solve",
        )(place, near, away, kept, partner)
    )


def solution(mesh):
    placed = (P("orb", "grid"), P("orb"))
    return jax.shard_map(
        on_device,
        mesh=mesh,
        in_specs=placed,
        out_specs=(P("orb", "grid"), P("orb", "grid")),
        check_vma=False,
    )
```

```python
import functools
import math

import jax
import jax.numpy as jnp
import numpy as np
from jax import lax
from jax.experimental import pallas as pl
from jax.experimental.pallas import tpu as pltpu
from jax.sharding import PartitionSpec as P

NX = 20
NY = 24
NZ = 24
NPTS = NX * NY * NZ
PLANE = NY * NZ
BAND = 128 // NZ
BANDS = -(-NY // BAND)
WIDE = BANDS * 128
F32 = jnp.float32
BF16 = jnp.bfloat16


def hartley_table(length):
    index = np.arange(length)
    angle = 2.0 * np.pi / length * (index[:, None] * index[None, :] % length)
    return (np.cos(angle) + np.sin(angle)).astype(BF16).astype(np.float32)


def signed_square(length):
    index = np.arange(length)
    signed = np.where(index <= length // 2, index, index - length)
    return (2.0 * np.pi * signed / length) ** 2


def coulomb_kernel():
    total = (
        signed_square(NX)[:, None, None]
        + signed_square(NY)[None, :, None]
        + signed_square(NZ)[None, None, :]
    )
    safe = np.where(total > 0, total, 1.0)
    return np.where(total > 0, 1.0 / safe, 0.0) / NPTS


def row_stride(own, planes):
    stride = planes + 1
    while own * stride % 8:
        stride += 1
    return stride


def tables(own, parts, cluster):
    planes = NX // parts
    stride = row_stride(own, planes)
    rows = own * stride
    table_x, table_y, table_z = hartley_table(NX), hartley_table(NY), hartley_table(NZ)
    mix_x = np.zeros((parts,) + (parts, cluster, own, stride) * 2, np.float32)
    cut = table_x.reshape(parts, planes, parts, planes)
    for part in range(parts):
        order = [part ^ other for other in range(parts)]
        for owner in range(cluster):
            for orbital in range(own):
                mix_x[part, :, owner, orbital, :planes, :, owner, orbital, :planes] = cut[
                    order
                ][:, :, order].transpose(0, 1, 2, 3)
    mix_x = mix_x.reshape(parts, cluster * parts * rows, cluster * parts * rows)
    lane = np.arange(NY)[:, None] // BAND * 128 + np.arange(NY)[:, None] % BAND * NZ + np.arange(NZ)
    mix_y = np.zeros((PLANE, WIDE), np.float32)
    natural = np.arange(PLANE).reshape(NY, NZ)
    for z in range(NZ):
        mix_y[np.ix_(natural[:, z], lane[:, z])] = table_y
    mix_z = np.zeros((256, 256), np.float32)
    for half in range(2):
        for band in range(BAND):
            at = half * 128 + band * NZ
            mix_z[at : at + NZ, at : at + NZ] = table_z
    scale = np.zeros((parts, own, stride, WIDE), np.float32)
    scale[:, :, :planes, lane.reshape(-1)] = coulomb_kernel().reshape(parts, 1, planes, PLANE)
    return (
        mix_x.astype(BF16),
        mix_y.astype(BF16),
        mix_z.astype(BF16),
        np.ascontiguousarray(mix_y.T).astype(BF16),
        scale.reshape(parts, rows, WIDE),
    )


def dot(left, right):
    return lax.dot_general(left, right, (((1,), (0,)), ((), ())), preferred_element_type=F32)


def bands(sections, mix_z):
    pieces = []
    for start in range(0, WIDE, 256):
        stop = min(start + 256, WIDE)
        width = stop - start
        pieces.append(dot(sections[:, start:stop], mix_z[:width, :width]))
    return jnp.concatenate(pieces, axis=1)


def halves(block, stride):
    return jnp.concatenate([block[..., stride:, :], block[..., :stride, :]], axis=-2)


class Route:
    def __init__(self, devices):
        top = devices.bit_length() - 1
        rest = list(range(top - 1, 1, -1))
        rounds = [rest[:2][::-1], rest[2:3] + [0]]
        rounds += [rest[at : at + 2] for at in range(3, len(rest), 2)] + [[1]]
        self.devices = devices
        self.rounds = rounds
        self.bits = [bit for members in rounds for bit in reversed(members)]
        self.owner_bits = [bit - 1 for bit in self.bits if bit]
        self.cluster = 1 << len(rounds[0])

    def masks(self, members):
        order = list(reversed(members))
        return [
            sum((at >> t & 1) << bit for t, bit in enumerate(order))
            for at in range(1 << len(order))
        ]

    def swap(self, array, mask):
        pairs = [(at, at ^ mask) for at in range(self.devices)]
        return lax.ppermute(array, ("orb", "grid"), pairs)


def spell(position, bits):
    return sum((position >> t & 1) << bit for t, bit in enumerate(bits))


def pack_body(orbitals, occupation, block, *, own, planes, stride):
    values = orbitals[...].astype(F32)
    weights = occupation[...].astype(F32)
    lines = []
    for orbital in range(own):
        for x in range(planes):
            lines.append(values[orbital : orbital + 1, x * PLANE : (x + 1) * PLANE])
        lines.append(
            jnp.broadcast_to(weights[:, orbital : orbital + 1], (stride - planes, PLANE))
        )
    block[0] = jnp.concatenate(lines, axis=0).astype(BF16)


def target_of(part, local, own, stride, cluster):
    mine = jnp.stack([local[0], local[cluster]]).astype(F32)
    first = lax.broadcasted_iota(jnp.int32, mine.shape, 1) < stride
    return jnp.where(first == (part == 0), mine, halves(mine, stride))


def sources_of(blocks, index, chunk, parts, cluster):
    source = blocks[pl.ds(index * chunk, chunk)].astype(F32)
    return source.reshape((chunk // (parts * cluster), parts, cluster) + blocks.shape[1:])


def add_pairs(
    part, target, blocks, mix_x, mix_y, mix_z, mix_back, scale, totals,
    *, parts, stride, planes, cluster, chunk,
):
    rows = blocks.shape[1]
    group = parts * cluster * rows
    first = lax.broadcasted_iota(jnp.int32, (1, 1, 1, rows, PLANE), 3) < stride
    x_table = mix_x[part]
    z_table = mix_z[...]
    factor = jnp.stack([scale[part], scale[1 - part]])[None, :, None]

    def step(index, carry):
        source = sources_of(blocks, index, chunk, parts, cluster)
        shape = source.shape[:-1]
        height = chunk * rows
        density = (source * target[None, :, None]).astype(BF16).reshape(height, PLANE)
        section = jnp.concatenate(
            [
                dot(x_table, density[at : at + group]).astype(BF16)
                for at in range(0, height, group)
            ]
        )
        section = dot(section, mix_y[...]).astype(BF16)
        spectrum = bands(section, z_table).reshape(shape + (WIDE,))
        section = (spectrum * factor).astype(BF16).reshape(height, WIDE)
        section = bands(section, z_table).astype(BF16)
        section = dot(section, mix_back[...]).astype(BF16)
        potential = jnp.concatenate(
            [dot(x_table, section[at : at + group]) for at in range(0, height, group)]
        ).reshape(shape + (PLANE,))
        weight = jnp.where(
            first,
            source[..., planes : planes + 1, :],
            source[..., stride + planes : stride + planes + 1, :],
        )
        totals[...] -= jnp.sum(weight * potential * source, axis=(0, 2))
        return carry

    steps = blocks.shape[0] // chunk
    if steps == 1:
        step(0, 0)
    else:
        lax.fori_loop(0, steps, step, 0)


def first_body(place, local, mix_x, mix_y, mix_z, mix_back, scale, totals, *, own, **sizes):
    target = target_of(place[1], local, own, sizes["stride"], sizes["cluster"])
    totals[...] = jnp.zeros_like(totals)
    add_pairs(
        place[1], target, local, mix_x, mix_y, mix_z, mix_back, scale, totals, **sizes
    )


def second_body(
    place, local, other, mix_x, mix_y, mix_z, mix_back, scale, before, sent, kept, totals,
    *, own, owner_bits, **sizes,
):
    stride, planes = sizes["stride"], sizes["planes"]
    parts, cluster, chunk = sizes["parts"], sizes["cluster"], sizes["chunk"]
    target = target_of(place[1], local, own, stride, cluster)
    totals[...] = before[...]
    add_pairs(
        place[1], target, other, mix_x, mix_y, mix_z, mix_back, scale, totals, **sizes
    )
    partial = totals[...]
    folded = partial + halves(partial, stride)
    rows = own * stride
    count = chunk // parts
    half = local.shape[0] // parts
    norb = 2 * half * own
    lane = lax.broadcasted_iota(jnp.int32, (count, norb), 1)
    slot = lax.broadcasted_iota(jnp.int32, (count, norb), 0)
    first = lax.broadcasted_iota(jnp.int32, (count, rows, PLANE), 1) < stride

    def overlap(blocks, base):
        def step(index, line):
            source = sources_of(blocks, index, chunk, parts, cluster)
            product = jnp.sum(source * folded[None, :, None], axis=1).reshape(count, rows, PLANE)
            owner = spell(base + index * count + slot, owner_bits) ^ place[0]
            for orbital in range(own):
                wanted = first if orbital == 0 else jnp.logical_not(first)
                picked = jnp.sum(jnp.where(wanted, product, 0.0), axis=1)
                value = jnp.sum(picked, axis=1, keepdims=True) / NPTS
                at = owner * own + orbital
                line = line + jnp.sum(jnp.where(lane == at, value, 0.0), axis=0, keepdims=True)
            return line

        return step

    line = jnp.zeros((1, norb), F32)
    steps = local.shape[0] // chunk
    for blocks, base in ((local, 0), (other, half)):
        step = overlap(blocks, base)
        line = step(0, line) if steps == 1 else lax.fori_loop(0, steps, step, line)
    line = jnp.concatenate([line, jnp.zeros((1, PLANE - norb), F32)], axis=1)
    high = line.astype(BF16).astype(F32)
    middle = (line - high).astype(BF16).astype(F32)
    low = line - high - middle
    height = sent.shape[1]
    row = lax.broadcasted_iota(jnp.int32, (1, height, PLANE), 1)
    mixed = folded[:, :height]
    for at, value in enumerate((high, middle, low)):
        mixed = jnp.where(row == planes + at, value[None], mixed)
    sent[...] = mixed.astype(BF16)
    kept[...] = folded[:, :height]


def solve_body(
    place, local, other, kept, partner, potentials, projectors, lines, work, weights,
    *, own, planes, bits, cluster,
):
    norb = lines.shape[0]
    half = norb // 2
    me = place[2]
    for blocks, base in ((local, 0), (other, half)):
        raw = blocks[:, :, :norb].astype(F32)
        lines[base : base + half] = (
            raw[:, planes] + raw[:, planes + 1] + raw[:, planes + 2]
        )

    def repeat(step):
        if norb <= 32:
            for at in range(norb):
                step(at)
        else:
            lax.fori_loop(0, norb, lambda at, carry: (step(at), carry)[1], 0)

    def settle(at):
        work[0, pl.ds(spell(at, bits) ^ me, 1), :] = lines[pl.ds(at, 1), :]

    repeat(settle)
    gram = work[0]
    left = -0.5 * (gram + gram.T)
    row = lax.broadcasted_iota(jnp.int32, (norb, norb), 0)
    column = lax.broadcasted_iota(jnp.int32, (norb, norb), 1)
    right = jnp.where(row == column, 1.0, 0.0).astype(F32)
    if norb <= 32:
        both = jnp.concatenate([left, right], axis=1)
        for k in range(norb):
            scaled = both[k : k + 1] / both[k : k + 1, k : k + 1]
            both = both - jnp.where(row[:, :1] > k, both[:, k : k + 1], 0.0) * scaled
        left, right = both[:, :norb], both[:, norb:]
    else:
        work[0] = left
        work[1] = right

        def step(k, carry):
            left = work[0]
            pivot_row = work[0, pl.ds(k, 1), :]
            right_row = work[1, pl.ds(k, 1), :]
            pivot = jnp.sum(jnp.where(column[:1] == k, pivot_row, 0.0), axis=1, keepdims=True)
            below = jnp.sum(jnp.where(column == k, left, 0.0), axis=1, keepdims=True)
            factor = jnp.where(row[:, :1] > k, below / pivot, 0.0)
            work[0] = left - factor * pivot_row
            work[1] = work[1] - factor * right_row
            return carry

        lax.fori_loop(0, norb, step, 0)
        left = work[0]
        right = work[1]
    diagonal = jnp.sum(jnp.where(row == column, left, 0.0), axis=1, keepdims=True)
    turned = (right * lax.rsqrt(diagonal)).T
    for orbital in range(own):
        at = place[0] * own + orbital
        value = jnp.sum(jnp.where(column == at, turned, 0.0), axis=1, keepdims=True)
        weights[orbital] = jnp.broadcast_to(value, (norb, PLANE))

    height = local.shape[1]
    own_values = kept[0]
    partner_values = partner[...]
    start = []
    for orbital in range(own):
        start.append(
            weights[orbital, pl.ds(me, 1), :] * (own_values - local[0].astype(F32))
            + weights[orbital, pl.ds(me ^ 1, 1), :]
            * (partner_values - local[cluster].astype(F32))
        )

    def gather(blocks, base):
        def step(at, sums):
            value = blocks[at].astype(F32)
            where = spell(base + at, bits) ^ me
            return tuple(
                sums[orbital] + weights[orbital, pl.ds(where, 1), :] * value
                for orbital in range(own)
            )

        return step

    sums = tuple(start)
    for blocks, base in ((local, 0), (other, half)):
        step = gather(blocks, base)
        if norb <= 32:
            for at in range(half):
                sums = step(at, sums)
        else:
            sums = lax.fori_loop(0, half, step, sums)
    second = place[1] == 1
    for orbital in range(own):
        swapped = second if orbital == 0 else jnp.logical_not(second)
        value = jnp.where(swapped, partner_values, own_values)
        for x in range(planes):
            lanes = slice(x * PLANE, (x + 1) * PLANE)
            potentials[orbital : orbital + 1, lanes] = value[x : x + 1]
            projectors[orbital : orbital + 1, lanes] = sums[orbital][x : x + 1]


def on_device(orbitals, occupation):
    own = orbitals.shape[0]
    owners = lax.axis_size("orb")
    parts = lax.axis_size("grid")
    devices = owners * parts
    planes = NX // parts
    stride = row_stride(own, planes)
    rows = own * stride
    route = Route(devices)
    cluster = route.cluster
    sizes = dict(parts=parts, stride=stride, planes=planes, cluster=cluster, chunk=16)
    orb, grid = lax.axis_index("orb"), lax.axis_index("grid")
    place = jnp.stack([orb, grid, orb * parts + grid]).astype(jnp.int32)
    vmem = pl.BlockSpec(memory_space=pltpu.VMEM)
    smem = pl.BlockSpec(memory_space=pltpu.SMEM)
    shape = jax.ShapeDtypeStruct
    mixing = [jnp.asarray(item) for item in tables(own, parts, cluster)]

    local = pl.pallas_call(
        functools.partial(pack_body, own=own, planes=planes, stride=stride),
        out_shape=shape((1, rows, PLANE), BF16),
        in_specs=[vmem, vmem],
        out_specs=vmem,
        name="pack",
    )(orbitals, occupation.reshape(1, own))
    for bit in reversed(route.rounds[0]):
        local = jnp.concatenate([local, route.swap(local, 1 << bit)])
    for members in route.rounds[1:-1]:
        local = jnp.concatenate(
            [local] + [route.swap(local, mask) for mask in route.masks(members)[1:]]
        )
    other = route.swap(local, route.masks(route.rounds[-1])[1])

    totals_shape = (parts, rows, PLANE)
    before = pl.pallas_call(
        functools.partial(first_body, own=own, **sizes),
        out_shape=shape(totals_shape, F32),
        in_specs=[smem] + [vmem] * 6,
        out_specs=vmem,
        name="near_pairs",
    )(place, local, *mixing)
    height = 16
    sent, kept = pl.pallas_call(
        functools.partial(second_body, own=own, owner_bits=route.owner_bits, **sizes),
        out_shape=(shape((parts, height, PLANE), BF16), shape((parts, height, PLANE), F32)),
        in_specs=[smem] + [vmem] * 8,
        out_specs=(vmem, vmem),
        scratch_shapes=[pltpu.VMEM(totals_shape, F32)],
        name="far_pairs",
    )(place, local, other, *mixing, before)

    column = sent[:, None]
    column = jnp.concatenate(
        [column] + [route.swap(column, mask) for mask in route.masks(route.rounds[0])[1:]], axis=1
    )
    partner = route.swap(kept[1], 1)
    column, partner = lax.optimization_barrier((column, partner))
    near, far = column[0], column[1]
    near = jnp.concatenate(
        [near]
        + [route.swap(far if mask & 1 else near, mask) for mask in route.masks(route.rounds[1])[1:]]
    )
    for members in route.rounds[2:-1]:
        near = jnp.concatenate(
            [near] + [route.swap(near, mask) for mask in route.masks(members)[1:]]
        )
    away = route.swap(near, route.masks(route.rounds[-1])[1])
    norb = devices
    size = planes * PLANE
    return tuple(
        pl.pallas_call(
            functools.partial(
                solve_body, own=own, planes=planes, bits=route.bits, cluster=cluster
            ),
            out_shape=(shape((own, size), F32), shape((own, size), F32)),
            in_specs=[smem] + [vmem] * 4,
            out_specs=(vmem, vmem),
            scratch_shapes=[
                pltpu.VMEM((norb, norb), F32),
                pltpu.VMEM((2, norb, norb), F32),
                pltpu.VMEM((own, norb, PLANE), F32),
            ],
            name="solve",
        )(place, near, away, kept, partner)
    )


def solution(mesh):
    placed = (P("orb", "grid"), P("orb"))
    return jax.shard_map(
        on_device,
        mesh=mesh,
        in_specs=placed,
        out_specs=(P("orb", "grid"), P("orb", "grid")),
        check_vma=False,
    )
```
